32 devices in a mesh: grp: 2 (over y), seg: 4 (over z), tile: 2 (over x), band: 2 (over core).
Axes of the slice: x: 2, y: 2, z: 4, core: 2. Of those that a mesh axis runs over, the one named last changes fastest.
Arguments:
- fields: float32 [6, 4, 128, 512], P(None, ('grp', 'tile'), None, 'seg'), parts along dimension 1, may hold values from 0 to 2400, as said below
- spectral_table: bfloat16 [128, 512], P(None, 'band'), may hold values from 0 to 0.0390625, as said below
- background: float32 [4, 128, 512], P(('grp', 'tile'), None, 'band'), parts along dimension 0, may hold values from 0.2 to 1
- active: int32 [4, 128], P(('grp', 'tile')), parts along dimension 0, may hold values 0 or 1
Outputs:
- radiance: float32 [4, 4, 128, 512], P('seg', ('grp', 'tile'), None, 'band'), parts along dimension 1
- band_mean: float32 [4, 4, 128], P('seg', ('grp', 'tile')), parts along dimension 1
The draws below stay inside these ranges and needn't reach their ends.
There are 2 independent parts, one for each index of `grp`. The reference program is written for one: setup_inputs(seed, part) draws one part's arguments, and reference() takes and returns one part's arrays. A program takes and returns all parts, laid end to end along the dimension named above; an argument that names none is the same for every part. Nothing has to cross between parts.
Inputs may be any that keep to these rules, and one draw needn't show every extreme that they name: fields[0] is a temperature in kelvin between 300 and 2400; fields[1:5] lie between 0.05 and 1; fields[5] lies between 0 and 0.7. `spectral_table`: every entry is positive.
All inputs are finite; a program needn't handle non-finite values. No bound on the sum of `active` on one device may be relied on, other than what follows from the above.
Results may differ from the reference program's by a relative error of at most 0.0003.
Values sent between devices are 32-bit elements; how exact they have to be, the bound alone decides.
A program may use at most 64 MiB of HBM per device.

```python
import math
import jax
import jax.numpy as jnp
from jax import lax

NW = 512
NB = 32
COLS = 128
F = 128
ROWS = 2
NZ = 512
N_SEG = 4


def draw_fields(key, part):
    stochastic_seeds = jax.random.split(jax.random.fold_in(key, 11), 5)
    grid_length = (ROWS, COLS, NZ)
    evenly_drawn_variate = jax.random.uniform(stochastic_seeds[0], grid_length, jnp.float32)
    species_draw = jax.random.uniform(stochastic_seeds[1], (4,) + grid_length, jnp.float32)
    thermal_distribution = 400.0 + 1800.0 * evenly_drawn_variate
    molar_share = jnp.exp(jnp.log(0.05) + species_draw * jnp.log(20.0))
    ambient_carbon_loading = jax.random.uniform(stochastic_seeds[2], grid_length, jnp.float32) * (0.2 / NZ)
    planes = jax.random.randint(stochastic_seeds[3], (3,), 0, NZ)
    sheet_intersection = jnp.any(jnp.arange(NZ)[:, None] == planes[None, :], axis=1)
    sudden_opacity_increment = jax.random.uniform(stochastic_seeds[4], grid_length, jnp.float32, 0.2, 0.7)
    carbon_opacity_depth = jnp.where(sheet_intersection[None, None, :], sudden_opacity_increment, ambient_carbon_loading)
    return jnp.concatenate([thermal_distribution[None], molar_share, carbon_opacity_depth[None]], 0).astype(jnp.float32)


def draw_spectral_table(key, part):
    stochastic_seeds = jax.random.split(jax.random.fold_in(key, 23), 2)
    low_log = jnp.log(0.05 / NZ)
    high_log = jnp.log(10.0 / NZ)
    strength = jnp.exp(low_log + (high_log - low_log) * jax.random.uniform(stochastic_seeds[0], (NW,), jnp.float32))
    factor = jax.random.uniform(stochastic_seeds[1], (F, NW), jnp.float32, 0.5, 1.5)
    return (strength[None, :] * factor).astype(jnp.bfloat16)


def with_ends(values, own_key, low, high):
    longest = values.shape.index(max(values.shape))
    spots = []
    for shift in (0, 1):
        where = [jax.random.randint(jax.random.fold_in(own_key, axis), (), 0, length) for axis, length in enumerate(values.shape)]
        where[longest] = (where[longest] + shift) % values.shape[longest]
        spots.append(tuple(where))
    return values.at[spots[0]].set(low).at[spots[1]].set(high)


def steps_of(key, extent, pieces, least, top_value):
    loudness = 1.0
    for position, shards_of in pieces:
        steps = jax.random.uniform(jax.random.fold_in(jax.random.fold_in(key, 6), position), (shards_of,), jnp.float32, least / len(pieces), top_value / len(pieces))
        loudness = loudness * jnp.repeat(jnp.exp(steps), extent[position] // shards_of).reshape((-1,) + (1,) * (len(extent) - 1 - position))
    return loudness


def setup_inputs(seed: int = 0, part: int = 0) -> dict:
    keys = jax.random.split(jax.random.key(seed), 5)
    part_keys = jax.random.split(jax.random.fold_in(keys[4], part), 5)
    fields = draw_fields(jax.random.fold_in(jax.random.fold_in(keys[4], part), 71), part)
    spectral_table = draw_spectral_table(jax.random.fold_in(keys[4], 71), part)
    background = jnp.clip(0.2 + 0.8 * jax.random.uniform(part_keys[2], (ROWS, COLS, NW), jnp.float32) ** steps_of(part_keys[2], (ROWS, COLS, NW), ((0, 2), (2, 2)), -0.2, 0.2), 0.2, 1.0)
    active = with_ends((jax.random.randint(part_keys[3], (ROWS, COLS), 0, 4) < 3).astype(jnp.int32), jax.random.fold_in(part_keys[3], 1), 0, 1)
    return {"fields": fields, "spectral_table": spectral_table, "background": background, "active": active}


boltzmann_ratio_term = 1.4388


def blackbody_intensity(spectral_line_position, thermal_distribution):
    nominal_magnitude = jnp.expm1(boltzmann_ratio_term * 2300.0 / 2000.0)
    return (spectral_line_position / 2300.0) ** 3 * nominal_magnitude / jnp.expm1(boltzmann_ratio_term * spectral_line_position / thermal_distribution)


def reference(fields, spectral_table, background, active):
    pixels = ROWS * COLS
    seg_cells = NZ // N_SEG
    flat = fields.reshape(6, pixels, NZ)
    back_flat = background.reshape(pixels, NW)
    active_flat = active.reshape(pixels).astype(jnp.float32)
    block_size = math.gcd(pixels, 16)
    block_count = pixels // block_size
    spectral_line_position = 2150.0 + 300.0 * (jnp.arange(NW, dtype=jnp.float32) + 0.5) / NW
    midway_locations = 300.0 + 2100.0 * jnp.arange(NB, dtype=jnp.float32) / (NB - 1)
    dispersion_multiplier = 2100.0 / (NB - 1)

    def one_block(index):
        start = (index * block_size).astype(jnp.int32)
        domain_tile_grids = lax.dynamic_slice_in_dim(flat, start, block_size, 1)
        back_block = lax.dynamic_slice_in_dim(back_flat, start, block_size, 0)
        active_block = lax.dynamic_slice_in_dim(active_flat, start, block_size, 0)
        thermal_distribution = domain_tile_grids[0]
        molar_share = domain_tile_grids[1:5]
        carbon_opacity_depth = domain_tile_grids[5]
        coordinate_directions = jnp.exp(-((thermal_distribution[None] - midway_locations[:, None, None]) / dispersion_multiplier) ** 2)
        features = (molar_share[:, None] * coordinate_directions[None]).reshape(F, block_size * NZ).astype(jnp.bfloat16)
        absorb = lax.dot_general(features, spectral_table, (((0,), (0,)), ((), ())), preferred_element_type=jnp.float32)
        voxel_opacity_depth = (absorb.reshape(block_size, NZ, NW) + carbon_opacity_depth[:, :, None]) * active_block[:, None, None]
        outgoing_intensity = -jnp.expm1(-voxel_opacity_depth) * blackbody_intensity(spectral_line_position[None, None, :], thermal_distribution[:, :, None])
        depth_four = voxel_opacity_depth.reshape(block_size, N_SEG, seg_cells, NW)
        emit_four = outgoing_intensity.reshape(block_size, N_SEG, seg_cells, NW)
        inclusive = jnp.flip(jnp.cumsum(jnp.flip(depth_four, 2), axis=2), 2)
        depth_after = inclusive - depth_four
        seg_source = jnp.sum(emit_four * jnp.exp(-depth_after), axis=2)
        seg_trans = jnp.exp(-inclusive[:, :, 0, :])
        seg_source = seg_source.at[:, 0].add(seg_trans[:, 0] * back_block)

        def advance(radiance_in, pair_now):
            radiance_out = pair_now[0] * radiance_in + pair_now[1]
            return radiance_out, radiance_out

        start_rad = jnp.zeros((block_size, NW), jnp.float32)
        _, leaving = lax.scan(advance, start_rad, (jnp.moveaxis(seg_trans, 1, 0), jnp.moveaxis(seg_source, 1, 0)))
        return leaving

    blocks = lax.map(one_block, jnp.arange(block_count, dtype=jnp.int32))
    radiance = jnp.transpose(blocks, (1, 0, 2, 3)).reshape(N_SEG, ROWS, COLS, NW)
    band_mean = jnp.sum(radiance, axis=3) / NW
    return radiance, band_mean
```

```python
import functools
import math

import jax
import jax.numpy as jnp
from jax import lax
from jax.experimental import pallas as pl
from jax.experimental.pallas import tpu as pltpu
from jax.sharding import PartitionSpec as P

NB = 32
NS = 4
NF = NS * NB
EXTRA = 16
C2 = 1.4388
LOG2E = math.log2(math.e)
SUB = 8
BLOCK = 64
PAIRS = 4
MESH = pl.DeviceIdType.MESH


def prepare(fields_ref, table_ref, active_ref, table_t, weights, inv_t, ratio, ft, step_w):
    pixels = fields_ref.shape[1]
    cells = fields_ref.shape[2]
    table_t[:, :NF] = table_ref[...].astype(jnp.float32).T.astype(jnp.bfloat16)
    table_t[:, NF:] = jnp.ones((table_t.shape[0], EXTRA), jnp.bfloat16)
    on = active_ref[...].astype(jnp.float32)
    temperature = fields_ref[0].T
    ft[0] = temperature
    scaled = C2 / temperature
    inv_t[...] = scaled
    ratio[...] = jnp.exp(scaled * (SUB * step_w))
    for i in range(1, 6):
        ft[i] = fields_ref[i].T * on
    basis = lax.broadcasted_iota(jnp.int32, (NB, pixels), 0).astype(jnp.float32)
    centre = 300.0 + 2100.0 * basis / (NB - 1)
    row = lax.broadcasted_iota(jnp.int32, (EXTRA, pixels), 0)

    def one_pair(p, carry):
        for h in range(2):
            z = 2 * p + h
            lanes = pl.ds(h * pixels, pixels)
            u = (ft[0, pl.ds(z, 1), :] - centre) * ((NB - 1) / 2100.0)
            bump = jnp.exp(-(u * u))
            for s in range(NS):
                feature = ft[1 + s, pl.ds(z, 1), :] * bump
                weights[p, s * NB : (s + 1) * NB, lanes] = feature.astype(jnp.bfloat16)
            soot = jnp.broadcast_to(ft[5, pl.ds(z, 1), :], (EXTRA, pixels))
            high = soot.astype(jnp.bfloat16).astype(jnp.float32)
            rest = soot - high
            mid = rest.astype(jnp.bfloat16).astype(jnp.float32)
            low = rest - mid
            piece = jnp.where(row == 0, high, jnp.where(row == 1, mid, jnp.where(row == 2, low, 0.0)))
            weights[p, NF:, lanes] = piece.astype(jnp.bfloat16)
        return carry

    lax.fori_loop(0, cells // 2, one_pair, 0)


def compute_block(block, wave0, step_w, table_t, weights, inv_t, ratio, depth, trans, source):
    pixels = inv_t.shape[1]
    chunks = inv_t.shape[0] // (2 * PAIRS)
    groups = BLOCK // SUB
    first = pl.multiple_of(block * BLOCK, BLOCK)
    lhs_rows = pl.ds(first, BLOCK)
    sub = lax.broadcasted_iota(jnp.int32, (SUB, pixels), 0)
    wave = wave0 + step_w * (sub + first).astype(jnp.float32)

    def multiply(q, buf):
        for p in range(PAIRS):
            buf[p] = jnp.dot(
                table_t[lhs_rows, :],
                weights[(chunks - 1 - q) * PAIRS + p],
                preferred_element_type=jnp.float32,
            )

    def march(q, buf, carry):
        total, behind, acc = (list(c) for c in carry)
        base = (chunks - 1 - q) * (2 * PAIRS)
        for i in reversed(range(2 * PAIRS)):
            p, h = divmod(i, 2)
            grow = jnp.exp(wave * inv_t[pl.ds(base + i, 1), :])
            rate = jnp.broadcast_to(ratio[pl.ds(base + i, 1), :], (SUB, pixels))
            for g in range(groups):
                total[g] = total[g] + buf[p, g * SUB : (g + 1) * SUB, h * pixels : (h + 1) * pixels]
                now = jnp.exp2(total[g] * (-LOG2E))
                acc[g] = acc[g] + (behind[g] - now) * pl.reciprocal(grow - 1.0)
                behind[g] = now
                if g + 1 < groups:
                    grow = grow * rate
        return tuple(total), tuple(behind), tuple(acc)

    def two_chunks(i, carry):
        multiply(2 * i + 1, depth[1])
        carry = march(2 * i, depth[0], carry)
        multiply(jnp.minimum(2 * i + 2, chunks - 1), depth[0])
        return march(2 * i + 1, depth[1], carry)

    multiply(0, depth[0])
    zero = jnp.zeros((SUB, pixels), jnp.float32)
    one = jnp.ones((SUB, pixels), jnp.float32)
    start = ((zero,) * groups, (one,) * groups, (zero,) * groups)
    _, behind, acc = lax.fori_loop(0, chunks // 2, two_chunks, start)
    nominal = math.expm1(C2 * 2300.0 / 2000.0)
    for g in range(groups):
        rows = pl.ds(first + g * SUB, SUB)
        rel = (wave + step_w * (g * SUB)) * (1.0 / 2300.0)
        trans[rows, :] = behind[g]
        source[rows, :] = acc[g] * (rel * rel * rel * nominal)


def kernel(
    n_seg, n_band, width_all,
    fields_ref, table_ref, back_ref, active_ref,
    out_ref, mean_ref,
    table_t, weights, inv_t, ratio, ft, depth0, depth1, trans, source, enter, leave, part, parts,
    send_sem, recv_sem, msend, mrecv,
):
    me = lax.axis_index("seg")
    band = lax.axis_index("band")
    width = table_ref.shape[1]
    blocks = width // BLOCK
    step_w = 300.0 / width_all
    wave0 = 2150.0 + step_w * ((band * width).astype(jnp.float32) + 0.5)

    barrier = pltpu.get_barrier_semaphore()

    @pl.when(me > 0)
    def _():
        pl.semaphore_signal(barrier, inc=1, device_id={"seg": me - 1}, device_id_type=MESH)

    @pl.when(me < n_seg - 1)
    def _():
        pl.semaphore_signal(barrier, inc=1, device_id={"seg": me + 1}, device_id_type=MESH)

    for o in range(1, n_band):
        pl.semaphore_signal(
            barrier, inc=1, device_id={"band": lax.rem(band + o, n_band)}, device_id_type=MESH
        )

    prepare(fields_ref, table_ref, active_ref, table_t, weights, inv_t, ratio, ft, step_w)
    part[...] = jnp.zeros_like(part)

    def hop(b):
        rows = pl.ds(pl.multiple_of(b * BLOCK, BLOCK), BLOCK)
        return pltpu.make_async_remote_copy(
            src_ref=leave.at[rows],
            dst_ref=enter.at[rows],
            send_sem=send_sem.at[b],
            recv_sem=recv_sem.at[b],
            device_id={"seg": lax.rem(me + 1, n_seg)},
            device_id_type=MESH,
        )

    def chain(b, carry):
        @pl.when(me > 0)
        def _():
            hop(b).wait_recv()

        rows = pl.ds(pl.multiple_of(b * BLOCK, BLOCK), BLOCK)
        radiance = trans[rows, :] * enter[rows, :] + source[rows, :]
        leave[rows, :] = radiance

        @pl.when(me < n_seg - 1)
        def _():
            hop(b).start()

        part[...] += jnp.sum(radiance.reshape(BLOCK // SUB, SUB, -1), axis=0)
        return carry

    def one_block(t, carry):
        compute_block(
            t, wave0, step_w, table_t, weights, inv_t, ratio, (depth0, depth1), trans, source
        )

        @pl.when(t == 0)
        def _():
            near = (me > 0).astype(jnp.int32) + (me < n_seg - 1).astype(jnp.int32)
            pl.semaphore_wait(barrier, near + (n_band - 1))

        @pl.when(t >= me)
        def _():
            chain(t - me, 0)

        return carry

    @pl.when(me == 0)
    def _():
        enter[...] = back_ref[...].T

    lax.fori_loop(0, blocks, one_block, 0)
    lax.fori_loop(jnp.maximum(blocks - me, 0), blocks, chain, 0)

    def swap(o):
        return pltpu.make_async_remote_copy(
            src_ref=part,
            dst_ref=parts.at[o - 1],
            send_sem=msend.at[o - 1],
            recv_sem=mrecv.at[o - 1],
            device_id={"band": lax.rem(band + o, n_band)},
            device_id_type=MESH,
        )

    for o in range(1, n_band):
        swap(o).start()
    out_ref[...] = leave[...].T

    @pl.when(me < n_seg - 1)
    def _():
        lax.fori_loop(0, blocks, lambda b, c: (hop(b).wait_send(), c)[1], 0)

    total = part[...]
    for o in range(1, n_band):
        swap(o).wait_recv()
        total = total + parts[o - 1]
    mean_ref[...] = jnp.sum(total, axis=0, keepdims=True) * (1.0 / width_all)
    for o in range(1, n_band):
        swap(o).wait_send()


def per_device(n_seg, n_band, fields, spectral_table, background, active):
    rows, cols, cells = fields.shape[1:]
    pixels = rows * cols
    width = spectral_table.shape[1]
    width_all = width * n_band
    blocks = width // BLOCK
    vmem = pl.BlockSpec(memory_space=pltpu.VMEM)
    f32, bf16 = jnp.float32, jnp.bfloat16
    radiance, mean = pl.pallas_call(
        functools.partial(kernel, n_seg, n_band, width_all),
        out_shape=(
            jax.ShapeDtypeStruct((pixels, width), f32),
            jax.ShapeDtypeStruct((1, pixels), f32),
        ),
        in_specs=[vmem] * 4,
        out_specs=(vmem, vmem),
        scratch_shapes=[
            pltpu.VMEM((width, NF + EXTRA), bf16),
            pltpu.VMEM((cells // 2, NF + EXTRA, 2 * pixels), bf16),
            pltpu.VMEM((cells, pixels), f32),
            pltpu.VMEM((cells, pixels), f32),
            pltpu.VMEM((6, cells, pixels), f32),
            pltpu.VMEM((PAIRS, BLOCK, 2 * pixels), f32),
            pltpu.VMEM((PAIRS, BLOCK, 2 * pixels), f32),
            pltpu.VMEM((width, pixels), f32),
            pltpu.VMEM((width, pixels), f32),
            pltpu.VMEM((width, pixels), f32),
            pltpu.VMEM((width, pixels), f32),
            pltpu.VMEM((SUB, pixels), f32),
            pltpu.VMEM((max(n_band - 1, 1), SUB, pixels), f32),
            pltpu.SemaphoreType.DMA((blocks,)),
            pltpu.SemaphoreType.DMA((blocks,)),
            pltpu.SemaphoreType.DMA((max(n_band - 1, 1),)),
            pltpu.SemaphoreType.DMA((max(n_band - 1, 1),)),
        ],
        compiler_params=pltpu.CompilerParams(collective_id=0, has_side_effects=True),
        name="flame",
    )(
        fields.reshape(6, pixels, cells),
        spectral_table,
        background.reshape(pixels, width),
        active.reshape(1, pixels),
    )
    return radiance.reshape(1, rows, cols, width), mean.reshape(1, rows, cols)


def solution(mesh):
    placed = (
        P(None, ("grp", "tile"), None, "seg"),
        P(None, "band"),
        P(("grp", "tile"), None, "band"),
        P(("grp", "tile"), None),
    )
    return jax.shard_map(
        functools.partial(per_device, mesh.shape["seg"], mesh.shape["band"]),
        mesh=mesh,
        in_specs=placed,
        out_specs=(P("seg", ("grp", "tile"), None, "band"), P("seg", ("grp", "tile"), None)),
        check_vma=False,
    )
```

```python
import functools
import math

import jax
import jax.numpy as jnp
from jax import lax
from jax.experimental import pallas as pl
from jax.experimental.pallas import tpu as pltpu
from jax.sharding import PartitionSpec as P

NB = 32
NS = 4
NF = NS * NB
EXTRA = 16
C2 = 1.4388
LOG2E = math.log2(math.e)
SUB = 8
BLOCK = 64
PAIRS = 8
HOP = 16
MESH = pl.DeviceIdType.MESH


def prepare(fields_ref, table_ref, active_ref, table_t, weights, inv_t, ratio, ft, step_w):
    pixels = fields_ref.shape[1]
    cells = fields_ref.shape[2]
    table_t[:, :NF] = table_ref[...].astype(jnp.float32).T.astype(jnp.bfloat16)
    table_t[:, NF:] = jnp.ones((table_t.shape[0], EXTRA), jnp.bfloat16)
    on = active_ref[...].astype(jnp.float32)
    temperature = fields_ref[0].T
    ft[0] = temperature
    scaled = (C2 * LOG2E) / temperature
    inv_t[...] = scaled
    ratio[...] = jnp.exp2(scaled * (SUB * step_w))
    for i in range(1, 6):
        ft[i] = fields_ref[i].T * on
    basis = lax.broadcasted_iota(jnp.int32, (NB, pixels), 0).astype(jnp.float32)
    centre = 300.0 + 2100.0 * basis / (NB - 1)
    row = lax.broadcasted_iota(jnp.int32, (EXTRA, pixels), 0)

    def one_pair(p, carry):
        for h in range(2):
            z = 2 * p + h
            lanes = pl.ds(h * pixels, pixels)
            u = (ft[0, pl.ds(z, 1), :] - centre) * ((NB - 1) / 2100.0)
            bump = jnp.exp(-(u * u))
            for s in range(NS):
                feature = ft[1 + s, pl.ds(z, 1), :] * bump
                weights[p, s * NB : (s + 1) * NB, lanes] = feature.astype(jnp.bfloat16)
            soot = jnp.broadcast_to(ft[5, pl.ds(z, 1), :], (EXTRA, pixels))
            high = soot.astype(jnp.bfloat16).astype(jnp.float32)
            rest = soot - high
            mid = rest.astype(jnp.bfloat16).astype(jnp.float32)
            low = rest - mid
            piece = jnp.where(row == 0, high, jnp.where(row == 1, mid, jnp.where(row == 2, low, 0.0)))
            weights[p, NF:, lanes] = piece.astype(jnp.bfloat16)
        return carry

    lax.fori_loop(0, cells // 2, one_pair, 0, unroll=4)


def compute_block(block, wave0, step_w, table_t, weights, inv_t, ratio, depth, trans, source):
    pixels = inv_t.shape[1]
    chunks = inv_t.shape[0] // (2 * PAIRS)
    groups = BLOCK // SUB
    first = pl.multiple_of(block * BLOCK, BLOCK)
    lhs_rows = pl.ds(first, BLOCK)
    sub = lax.broadcasted_iota(jnp.int32, (SUB, pixels), 0)
    wave = wave0 + step_w * (sub + first).astype(jnp.float32)

    def multiply(q, buf):
        for p in range(PAIRS):
            buf[p] = jnp.dot(
                table_t[lhs_rows, :],
                weights[(chunks - 1 - q) * PAIRS + p],
                preferred_element_type=jnp.float32,
            )

    def march(q, buf, carry):
        total, behind, acc = (list(c) for c in carry)
        base = (chunks - 1 - q) * (2 * PAIRS)
        for i in reversed(range(2 * PAIRS)):
            p, h = divmod(i, 2)
            grow = jnp.exp2(wave * inv_t[pl.ds(base + i, 1), :])
            rate = jnp.broadcast_to(ratio[pl.ds(base + i, 1), :], (SUB, pixels))
            for g in range(groups):
                total[g] = total[g] + buf[p, g * SUB : (g + 1) * SUB, h * pixels : (h + 1) * pixels]
                now = jnp.exp2(total[g] * (-LOG2E))
                acc[g] = acc[g] + (behind[g] - now) * pl.reciprocal(grow - 1.0)
                behind[g] = now
                if g + 1 < groups:
                    grow = grow * rate
        return tuple(total), tuple(behind), tuple(acc)

    def two_chunks(i, carry):
        multiply(2 * i + 1, depth[1])
        carry = march(2 * i, depth[0], carry)
        multiply(jnp.minimum(2 * i + 2, chunks - 1), depth[0])
        return march(2 * i + 1, depth[1], carry)

    multiply(0, depth[0])
    zero = jnp.zeros((SUB, pixels), jnp.float32)
    one = jnp.ones((SUB, pixels), jnp.float32)
    start = ((zero,) * groups, (one,) * groups, (zero,) * groups)
    _, behind, acc = lax.fori_loop(0, chunks // 2, two_chunks, start)
    nominal = math.expm1(C2 * 2300.0 / 2000.0)
    for g in range(groups):
        rows = pl.ds(first + g * SUB, SUB)
        rel = (wave + step_w * (g * SUB)) * (1.0 / 2300.0)
        trans[rows, :] = behind[g]
        source[rows, :] = acc[g] * (rel * rel * rel * nominal)


def kernel(
    n_seg, n_band, width_all,
    fields_ref, table_ref, back_ref, active_ref,
    out_ref, mean_ref,
    table_t, weights, inv_t, ratio, ft, depth0, depth1, trans, source, enter, leave, part, parts,
    send_sem, recv_sem, msend, mrecv,
):
    me = lax.axis_index("seg")
    band = lax.axis_index("band")
    width = table_ref.shape[1]
    blocks = width // BLOCK
    per = BLOCK // HOP
    step_w = 300.0 / width_all
    wave0 = 2150.0 + step_w * ((band * width).astype(jnp.float32) + 0.5)

    barrier = pltpu.get_barrier_semaphore()

    @pl.when(me > 0)
    def _():
        pl.semaphore_signal(barrier, inc=1, device_id={"seg": me - 1}, device_id_type=MESH)

    @pl.when(me < n_seg - 1)
    def _():
        pl.semaphore_signal(barrier, inc=1, device_id={"seg": me + 1}, device_id_type=MESH)

    for o in range(1, n_band):
        pl.semaphore_signal(
            barrier, inc=1, device_id={"band": lax.rem(band + o, n_band)}, device_id_type=MESH
        )

    prepare(fields_ref, table_ref, active_ref, table_t, weights, inv_t, ratio, ft, step_w)
    part[...] = jnp.zeros_like(part)

    def hop(u):
        rows = pl.ds(pl.multiple_of(u * HOP, HOP), HOP)
        return pltpu.make_async_remote_copy(
            src_ref=leave.at[rows],
            dst_ref=enter.at[rows],
            send_sem=send_sem.at[u],
            recv_sem=recv_sem.at[u],
            device_id={"seg": lax.rem(me + 1, n_seg)},
            device_id_type=MESH,
        )

    def chain(u, carry):
        @pl.when(me > 0)
        def _():
            hop(u).wait_recv()

        rows = pl.ds(pl.multiple_of(u * HOP, HOP), HOP)
        radiance = trans[rows, :] * enter[rows, :] + source[rows, :]
        leave[rows, :] = radiance

        @pl.when(me < n_seg - 1)
        def _():
            hop(u).start()

        part[...] += jnp.sum(radiance.reshape(HOP // SUB, SUB, -1), axis=0)
        return carry

    def one_block(t, carry):
        compute_block(
            t, wave0, step_w, table_t, weights, inv_t, ratio, (depth0, depth1), trans, source
        )

        @pl.when(t == 0)
        def _():
            near = (me > 0).astype(jnp.int32) + (me < n_seg - 1).astype(jnp.int32)
            pl.semaphore_wait(barrier, near + (n_band - 1))

        @pl.when(t >= me)
        def _():
            lax.fori_loop((t - me) * per, (t - me + 1) * per, chain, 0)

        return carry

    @pl.when(me == 0)
    def _():
        enter[...] = back_ref[...].T

    lax.fori_loop(0, blocks, one_block, 0)
    lax.fori_loop(jnp.maximum(blocks - me, 0) * per, blocks * per, chain, 0)

    def swap(o):
        return pltpu.make_async_remote_copy(
            src_ref=part,
            dst_ref=parts.at[o - 1],
            send_sem=msend.at[o - 1],
            recv_sem=mrecv.at[o - 1],
            device_id={"band": lax.rem(band + o, n_band)},
            device_id_type=MESH,
        )

    for o in range(1, n_band):
        swap(o).start()
    out_ref[...] = leave[...].T

    @pl.when(me < n_seg - 1)
    def _():
        lax.fori_loop(0, blocks * per, lambda u, c: (hop(u).wait_send(), c)[1], 0)

    total = part[...]
    for o in range(1, n_band):
        swap(o).wait_recv()
        total = total + parts[o - 1]
    mean_ref[...] = jnp.sum(total, axis=0, keepdims=True) * (1.0 / width_all)
    for o in range(1, n_band):
        swap(o).wait_send()


def per_device(n_seg, n_band, fields, spectral_table, background, active):
    rows, cols, cells = fields.shape[1:]
    pixels = rows * cols
    width = spectral_table.shape[1]
    width_all = width * n_band
    hops = width // HOP
    vmem = pl.BlockSpec(memory_space=pltpu.VMEM)
    f32, bf16 = jnp.float32, jnp.bfloat16
    radiance, mean = pl.pallas_call(
        functools.partial(kernel, n_seg, n_band, width_all),
        out_shape=(
            jax.ShapeDtypeStruct((pixels, width), f32),
            jax.ShapeDtypeStruct((1, pixels), f32),
        ),
        in_specs=[vmem] * 4,
        out_specs=(vmem, vmem),
        scratch_shapes=[
            pltpu.VMEM((width, NF + EXTRA), bf16),
            pltpu.VMEM((cells // 2, NF + EXTRA, 2 * pixels), bf16),
            pltpu.VMEM((cells, pixels), f32),
            pltpu.VMEM((cells, pixels), f32),
            pltpu.VMEM((6, cells, pixels), f32),
            pltpu.VMEM((PAIRS, BLOCK, 2 * pixels), f32),
            pltpu.VMEM((PAIRS, BLOCK, 2 * pixels), f32),
            pltpu.VMEM((width, pixels), f32),
            pltpu.VMEM((width, pixels), f32),
            pltpu.VMEM((width, pixels), f32),
            pltpu.VMEM((width, pixels), f32),
            pltpu.VMEM((SUB, pixels), f32),
            pltpu.VMEM((max(n_band - 1, 1), SUB, pixels), f32),
            pltpu.SemaphoreType.DMA((hops,)),
            pltpu.SemaphoreType.DMA((hops,)),
            pltpu.SemaphoreType.DMA((max(n_band - 1, 1),)),
            pltpu.SemaphoreType.DMA((max(n_band - 1, 1),)),
        ],
        compiler_params=pltpu.CompilerParams(collective_id=0, has_side_effects=True, vmem_limit_bytes=24 * 2**20),
        name="flame",
    )(
        fields.reshape(6, pixels, cells),
        spectral_table,
        background.reshape(pixels, width),
        active.reshape(1, pixels),
    )
    return radiance.reshape(1, rows, cols, width), mean.reshape(1, rows, cols)


def solution(mesh):
    placed = (
        P(None, ("grp", "tile"), None, "seg"),
        P(None, "band"),
        P(("grp", "tile"), None, "band"),
        P(("grp", "tile"), None),
    )
    return jax.shard_map(
        functools.partial(per_device, mesh.shape["seg"], mesh.shape["band"]),
        mesh=mesh,
        in_specs=placed,
        out_specs=(P("seg", ("grp", "tile"), None, "band"), P("seg", ("grp", "tile"), None)),
        check_vma=False,
    )
```

```python
import functools
import math

import jax
import jax.numpy as jnp
from jax import lax
from jax.experimental import pallas as pl
from jax.experimental.pallas import tpu as pltpu
from jax.sharding import PartitionSpec as P

NB = 32
NS = 4
NF = NS * NB
EXTRA = 16
C2 = 1.4388
LOG2E = math.log2(math.e)
SUB = 8
BLOCK = 64
PAIRS = 8
HOP = 16
MESH = pl.DeviceIdType.MESH


def prepare(fields_ref, table_ref, active_ref, table_t, weights, inv_t, ratio, ft, step_w):
    pixels = fields_ref.shape[1]
    cells = fields_ref.shape[2]
    table_t[:, :NF] = table_ref[...].astype(jnp.float32).T.astype(jnp.bfloat16)
    table_t[:, NF:] = jnp.ones((table_t.shape[0], EXTRA), jnp.bfloat16)
    on = active_ref[...].astype(jnp.float32)
    temperature = fields_ref[0].T
    ft[0] = temperature
    scaled = (C2 * LOG2E) / temperature
    inv_t[...] = scaled
    ratio[...] = jnp.exp2(scaled * (SUB * step_w))
    for i in range(1, 6):
        ft[i] = fields_ref[i].T * on
    basis = lax.broadcasted_iota(jnp.int32, (NB, pixels), 0).astype(jnp.float32)
    centre = 300.0 + 2100.0 * basis / (NB - 1)
    row = lax.broadcasted_iota(jnp.int32, (EXTRA, pixels), 0)

    def one_pair(p, carry):
        for h in range(2):
            z = 2 * p + h
            lanes = pl.ds(h * pixels, pixels)
            u = (ft[0, pl.ds(z, 1), :] - centre) * ((NB - 1) / 2100.0)
            bump = jnp.exp(-(u * u))
            for s in range(NS):
                feature = ft[1 + s, pl.ds(z, 1), :] * bump
                weights[p, s * NB : (s + 1) * NB, lanes] = feature.astype(jnp.bfloat16)
            soot = jnp.broadcast_to(ft[5, pl.ds(z, 1), :], (EXTRA, pixels))
            high = soot.astype(jnp.bfloat16).astype(jnp.float32)
            rest = soot - high
            mid = rest.astype(jnp.bfloat16).astype(jnp.float32)
            low = rest - mid
            piece = jnp.where(row == 0, high, jnp.where(row == 1, mid, jnp.where(row == 2, low, 0.0)))
            weights[p, NF:, lanes] = piece.astype(jnp.bfloat16)
        return carry

    lax.fori_loop(0, cells // 2, one_pair, 0, unroll=4)


def compute_block(block, wave0, step_w, table_t, weights, inv_t, ratio, depth, trans, source):
    pixels = inv_t.shape[1]
    chunks = inv_t.shape[0] // (2 * PAIRS)
    groups = BLOCK // SUB
    first = pl.multiple_of(block * BLOCK, BLOCK)
    lhs_rows = pl.ds(first, BLOCK)
    sub = lax.broadcasted_iota(jnp.int32, (SUB, pixels), 0)
    wave = wave0 + step_w * (sub + first).astype(jnp.float32)

    def multiply(q, buf):
        for p in range(PAIRS):
            buf[p] = jnp.dot(
                table_t[lhs_rows, :],
                weights[(chunks - 1 - q) * PAIRS + p],
                preferred_element_type=jnp.float32,
            )

    def march(q, buf, carry):
        total, behind, acc = (list(c) for c in carry)
        base = (chunks - 1 - q) * (2 * PAIRS)
        for i in reversed(range(2 * PAIRS)):
            p, h = divmod(i, 2)
            grow = jnp.exp2(wave * inv_t[pl.ds(base + i, 1), :])
            rate = jnp.broadcast_to(ratio[pl.ds(base + i, 1), :], (SUB, pixels))
            for g in range(groups):
                total[g] = total[g] + buf[p, g * SUB : (g + 1) * SUB, h * pixels : (h + 1) * pixels]
                now = jnp.exp2(total[g] * (-LOG2E))
                acc[g] = acc[g] + (behind[g] - now) * pl.reciprocal(grow - 1.0)
                behind[g] = now
                if g + 1 < groups:
                    grow = grow * rate
        return tuple(total), tuple(behind), tuple(acc)

    def two_chunks(i, carry):
        multiply(2 * i + 1, depth[1])
        carry = march(2 * i, depth[0], carry)
        multiply(jnp.minimum(2 * i + 2, chunks - 1), depth[0])
        return march(2 * i + 1, depth[1], carry)

    multiply(0, depth[0])
    zero = jnp.zeros((SUB, pixels), jnp.float32)
    one = jnp.ones((SUB, pixels), jnp.float32)
    start = ((zero,) * groups, (one,) * groups, (zero,) * groups)
    _, behind, acc = lax.fori_loop(0, chunks // 2, two_chunks, start)
    nominal = math.expm1(C2 * 2300.0 / 2000.0)
    for g in range(groups):
        rows = pl.ds(first + g * SUB, SUB)
        rel = (wave + step_w * (g * SUB)) * (1.0 / 2300.0)
        trans[rows, :] = behind[g]
        source[rows, :] = acc[g] * (rel * rel * rel * nominal)


def kernel(
    n_seg, n_band, width_all,
    fields_hbm, table_hbm, back_hbm, active_hbm,
    out_ref, mean_ref,
    table_t, weights, inv_t, ratio, ft, depth0, depth1, trans, source, enter, leave, part, parts,
    fields_ref, table_ref, back_ref, active_ref, load_sem,
    send_sem, recv_sem, msend, mrecv,
):
    loads = [
        pltpu.make_async_copy(src, dst, load_sem.at[i])
        for i, (src, dst) in enumerate(
            (
                (fields_hbm, fields_ref),
                (active_hbm, active_ref),
                (table_hbm, table_ref),
                (back_hbm, back_ref),
            )
        )
    ]
    for load in loads:
        load.start()
    me = lax.axis_index("seg")
    band = lax.axis_index("band")
    width = table_ref.shape[1]
    blocks = width // BLOCK
    per = BLOCK // HOP
    step_w = 300.0 / width_all
    wave0 = 2150.0 + step_w * ((band * width).astype(jnp.float32) + 0.5)

    barrier = pltpu.get_barrier_semaphore()

    @pl.when(me > 0)
    def _():
        pl.semaphore_signal(barrier, inc=1, device_id={"seg": me - 1}, device_id_type=MESH)

    @pl.when(me < n_seg - 1)
    def _():
        pl.semaphore_signal(barrier, inc=1, device_id={"seg": me + 1}, device_id_type=MESH)

    for o in range(1, n_band):
        pl.semaphore_signal(
            barrier, inc=1, device_id={"band": lax.rem(band + o, n_band)}, device_id_type=MESH
        )

    for load in loads[:3]:
        load.wait()
    prepare(fields_ref, table_ref, active_ref, table_t, weights, inv_t, ratio, ft, step_w)
    part[...] = jnp.zeros_like(part)

    def hop(u):
        rows = pl.ds(pl.multiple_of(u * HOP, HOP), HOP)
        return pltpu.make_async_remote_copy(
            src_ref=leave.at[rows],
            dst_ref=enter.at[rows],
            send_sem=send_sem.at[u],
            recv_sem=recv_sem.at[u],
            device_id={"seg": lax.rem(me + 1, n_seg)},
            device_id_type=MESH,
        )

    def chain(u, carry):
        @pl.when(me > 0)
        def _():
            hop(u).wait_recv()

        rows = pl.ds(pl.multiple_of(u * HOP, HOP), HOP)
        radiance = trans[rows, :] * enter[rows, :] + source[rows, :]
        leave[rows, :] = radiance

        @pl.when(me < n_seg - 1)
        def _():
            hop(u).start()

        part[...] += jnp.sum(radiance.reshape(HOP // SUB, SUB, -1), axis=0)
        return carry

    def one_block(t, carry):
        compute_block(
            t, wave0, step_w, table_t, weights, inv_t, ratio, (depth0, depth1), trans, source
        )

        @pl.when(t == 0)
        def _():
            near = (me > 0).astype(jnp.int32) + (me < n_seg - 1).astype(jnp.int32)
            pl.semaphore_wait(barrier, near + (n_band - 1))

        @pl.when(t >= me)
        def _():
            lax.fori_loop((t - me) * per, (t - me + 1) * per, chain, 0)

        return carry

    loads[3].wait()

    @pl.when(me == 0)
    def _():
        enter[...] = back_ref[...].T

    lax.fori_loop(0, blocks, one_block, 0)
    lax.fori_loop(jnp.maximum(blocks - me, 0) * per, blocks * per, chain, 0)

    def swap(o):
        return pltpu.make_async_remote_copy(
            src_ref=part,
            dst_ref=parts.at[o - 1],
            send_sem=msend.at[o - 1],
            recv_sem=mrecv.at[o - 1],
            device_id={"band": lax.rem(band + o, n_band)},
            device_id_type=MESH,
        )

    for o in range(1, n_band):
        swap(o).start()
    out_ref[...] = leave[...].T

    @pl.when(me < n_seg - 1)
    def _():
        lax.fori_loop(0, blocks * per, lambda u, c: (hop(u).wait_send(), c)[1], 0)

    total = part[...]
    for o in range(1, n_band):
        swap(o).wait_recv()
        total = total + parts[o - 1]
    mean_ref[...] = jnp.sum(total, axis=0, keepdims=True) * (1.0 / width_all)
    for o in range(1, n_band):
        swap(o).wait_send()


def per_device(n_seg, n_band, fields, spectral_table, background, active):
    rows, cols, cells = fields.shape[1:]
    pixels = rows * cols
    width = spectral_table.shape[1]
    width_all = width * n_band
    hops = width // HOP
    vmem = pl.BlockSpec(memory_space=pltpu.VMEM)
    f32, bf16 = jnp.float32, jnp.bfloat16
    radiance, mean = pl.pallas_call(
        functools.partial(kernel, n_seg, n_band, width_all),
        out_shape=(
            jax.ShapeDtypeStruct((pixels, width), f32),
            jax.ShapeDtypeStruct((1, pixels), f32),
        ),
        in_specs=[pl.BlockSpec(memory_space=pltpu.HBM)] * 4,
        out_specs=(vmem, vmem),
        scratch_shapes=[
            pltpu.VMEM((width, NF + EXTRA), bf16),
            pltpu.VMEM((cells // 2, NF + EXTRA, 2 * pixels), bf16),
            pltpu.VMEM((cells, pixels), f32),
            pltpu.VMEM((cells, pixels), f32),
            pltpu.VMEM((6, cells, pixels), f32),
            pltpu.VMEM((PAIRS, BLOCK, 2 * pixels), f32),
            pltpu.VMEM((PAIRS, BLOCK, 2 * pixels), f32),
            pltpu.VMEM((width, pixels), f32),
            pltpu.VMEM((width, pixels), f32),
            pltpu.VMEM((width, pixels), f32),
            pltpu.VMEM((width, pixels), f32),
            pltpu.VMEM((SUB, pixels), f32),
            pltpu.VMEM((max(n_band - 1, 1), SUB, pixels), f32),
            pltpu.VMEM((6, pixels, cells), f32),
            pltpu.VMEM((NF, width), bf16),
            pltpu.VMEM((pixels, width), f32),
            pltpu.VMEM((1, pixels), jnp.int32),
            pltpu.SemaphoreType.DMA((4,)),
            pltpu.SemaphoreType.DMA((hops,)),
            pltpu.SemaphoreType.DMA((hops,)),
            pltpu.SemaphoreType.DMA((max(n_band - 1, 1),)),
            pltpu.SemaphoreType.DMA((max(n_band - 1, 1),)),
        ],
        compiler_params=pltpu.CompilerParams(collective_id=0, has_side_effects=True, vmem_limit_bytes=24 * 2**20),
        name="flame",
    )(
        pltpu.with_memory_space_constraint(fields.reshape(6, pixels, cells), pltpu.HBM),
        pltpu.with_memory_space_constraint(spectral_table, pltpu.HBM),
        pltpu.with_memory_space_constraint(background.reshape(pixels, width), pltpu.HBM),
        pltpu.with_memory_space_constraint(active.reshape(1, pixels), pltpu.HBM),
    )
    return radiance.reshape(1, rows, cols, width), mean.reshape(1, rows, cols)


def solution(mesh):
    placed = (
        P(None, ("grp", "tile"), None, "seg"),
        P(None, "band"),
        P(("grp", "tile"), None, "band"),
        P(("grp", "tile"), None),
    )
    return jax.shard_map(
        functools.partial(per_device, mesh.shape["seg"], mesh.shape["band"]),
        mesh=mesh,
        in_specs=placed,
        out_specs=(P("seg", ("grp", "tile"), None, "band"), P("seg", ("grp", "tile"), None)),
        check_vma=False,
    )
```
